64 devices in a mesh: rep: 8 (over x, y, core), dp: 8 (over z).
Axes of the slice: x: 2, y: 2, z: 8, core: 2. Of those that a mesh axis runs over, the one named last changes fastest.
The devices are a block of a 4x4x8 slice.
Arguments:
- x: bfloat16 [64, 2048, 512], P(('rep', 'dp')), parts along dimension 0
- dy: bfloat16 [64, 2048, 512], P(('rep', 'dp')), parts along dimension 0
- wq: bfloat16 [2, 512, 512], P(None, 'dp')
- wk: bfloat16 [2, 512, 128], P(None, 'dp')
- wv: bfloat16 [2, 512, 128], P(None, 'dp')
- wo: bfloat16 [2, 512, 512], P(None, 'dp')
- w_gate: bfloat16 [2, 512, 1536], P(None, 'dp')
- w_up: bfloat16 [2, 512, 1536], P(None, 'dp')
- w_down: bfloat16 [2, 1536, 512], P(None, 'dp')
Outputs:
- output 1: bfloat16 [64, 2048, 512], P(('rep', 'dp')), parts along dimension 0
- output 2: bfloat16 [16, 512, 512], P('rep', 'dp'), parts along dimension 0
- output 3: bfloat16 [16, 512, 128], P('rep', 'dp'), parts along dimension 0
- output 4: bfloat16 [16, 512, 128], P('rep', 'dp'), parts along dimension 0
- output 5: bfloat16 [16, 512, 512], P('rep', 'dp'), parts along dimension 0
- output 6: bfloat16 [16, 512, 1536], P('rep', 'dp'), parts along dimension 0
- output 7: bfloat16 [16, 512, 1536], P('rep', 'dp'), parts along dimension 0
- output 8: bfloat16 [16, 1536, 512], P('rep', 'dp'), parts along dimension 0
There are 8 independent parts. The reference program is written for one: setup_inputs(seed, part) draws one part's arguments, and reference() takes and returns one part's arrays. A program takes and returns all parts, laid end to end along the dimension named above; an argument that names none is the same for every part.
All inputs are finite; a program needn't handle non-finite values.
Results may differ from the reference program's by a relative error of at most 0.0269.
Values are sent between devices in bfloat16 or wider.
A program may use at most 768 MiB of HBM per device.

```python
import jax
import jax.numpy as jnp
from jax import lax

SEQUENCES = 8
TOKENS = 2048
D = 512
HEADS = 4
KV_HEADS = 1
HEAD = 128
FF = 1536
LAYERS = 2
THETA = 10000
NAMES = ("wq", "wk", "wv", "wo", "w_gate", "w_up", "w_down")
SHAPES = {
    "wq": (LAYERS, D, HEADS * HEAD),
    "wk": (LAYERS, D, KV_HEADS * HEAD),
    "wv": (LAYERS, D, KV_HEADS * HEAD),
    "wo": (LAYERS, HEADS * HEAD, D),
    "w_gate": (LAYERS, D, FF),
    "w_up": (LAYERS, D, FF),
    "w_down": (LAYERS, FF, D),
}


def bump(key, n, height):
    away = (jnp.arange(n, dtype=jnp.int32) - jax.random.randint(key, (), 0, n, jnp.int32)) % n
    return jnp.where(away < n // 8, height, 1.0)


def together(key, own, strength):
    shared = jax.random.normal(key, own.shape[1:], jnp.float32)
    return (own + strength * shared) * lax.rsqrt(1 + strength * strength)


def setup_inputs(seed: int = 0, part: int = 0) -> dict:
    kx, kdy, ka, kb, kz, kf, kh, kl, *keys = jax.random.split(jax.random.key(seed), 8 + 3 * len(NAMES))
    kx, kdy, ka, kb = (jax.random.fold_in(k, part) for k in (kx, kdy, ka, kb))
    kw, km, kv = (keys[i::3] for i in range(3))
    shape = (SEQUENCES, TOKENS, D)
    much_x, much_dy = jax.random.uniform(kz, (2,), jnp.float32, 0.0, 1.0)
    loud = 2.0 ** jax.random.uniform(jax.random.fold_in(kz, 1), (), jnp.float32, -1.0, 2.0)
    layers = 2.0 ** jax.random.uniform(kl, (LAYERS, 1, 1), jnp.float32, -1.0, 1.0)
    times = {"wq": 1.0, "wk": 1.0, "wv": 2.0, "wo": layers, "w_gate": 1.0, "w_up": bump(kh, FF, 4.0), "w_down": layers}
    x = together(ka, jax.random.normal(kx, shape, jnp.float32), much_x) * bump(kf, D, 4.0)
    dy = together(kb, jax.random.normal(kdy, shape, jnp.float32), much_dy)
    drawn = {"x": x.astype(jnp.bfloat16), "dy": (loud * dy * (SEQUENCES * TOKENS) ** -0.5).astype(jnp.bfloat16)}
    for key, name in zip(kw, NAMES, strict=True):
        drawn[name] = (jax.random.normal(key, SHAPES[name], jnp.float32) * SHAPES[name][1] ** -0.5 * times[name]).astype(jnp.bfloat16)
    return drawn


def matmul(a, w):
    return jnp.dot(a, w, preferred_element_type=jnp.float32).astype(jnp.bfloat16)


def normed(h):
    wide = h.astype(jnp.float32)
    scale = lax.rsqrt(jnp.mean(wide**2, -1, keepdims=True) + 1e-6)
    return (wide * scale).astype(jnp.bfloat16)


def turned(t, theta):
    half = t.shape[-1] // 2
    angle = jnp.arange(t.shape[0], dtype=jnp.float32)[:, None] * theta ** (-jnp.arange(half, dtype=jnp.float32) / half)
    cos, sin = jnp.cos(angle)[:, None], jnp.sin(angle)[:, None]
    a, b = t[..., :half].astype(jnp.float32), t[..., half:].astype(jnp.float32)
    return jnp.concatenate([a * cos - b * sin, b * cos + a * sin], -1).astype(jnp.bfloat16)


def seen_by(q, k, v):
    tokens, kv = q.shape[0], k.shape[1]
    q = q.reshape(tokens, kv, -1, q.shape[-1])
    scores = jnp.einsum("tgsd,ugd->gstu", q.astype(jnp.float32), k.astype(jnp.float32)) * q.shape[-1] ** -0.5
    place = jnp.arange(tokens)
    weights = jax.nn.softmax(jnp.where(place[:, None] >= place, scores, -jnp.inf), -1).astype(jnp.bfloat16)
    return jnp.einsum("gstu,ugd->tgsd", weights.astype(jnp.float32), v.astype(jnp.float32)).astype(jnp.bfloat16).reshape(tokens, -1)


def layer(h, w):
    a = normed(h)
    q, k = (turned(matmul(a, w[name]).reshape(h.shape[0], -1, HEAD), THETA) for name in ("wq", "wk"))
    h = h + matmul(seen_by(q, k, matmul(a, w["wv"]).reshape(h.shape[0], -1, HEAD)), w["wo"])
    b = normed(h)
    gate = jnp.dot(b, w["w_gate"], preferred_element_type=jnp.float32)
    up = jnp.dot(b, w["w_up"], preferred_element_type=jnp.float32)
    return h + matmul((jax.nn.silu(gate) * up).astype(jnp.bfloat16), w["w_down"])


def stack(weights, h):
    return lax.scan(lambda h, w: (layer(h, w), None), h, weights)[0]


def reference(x, dy, wq, wk, wv, wo, w_gate, w_up, w_down):
    weights = dict(zip(NAMES, (wq, wk, wv, wo, w_gate, w_up, w_down), strict=True))

    def take(so_far, sequence):
        h, by_y = sequence
        _, back = jax.vjp(stack, weights, h)
        by_weights, by_h = back(by_y)
        return jax.tree.map(lambda total, term: total + term.astype(jnp.float32), so_far, by_weights), by_h

    none_yet = {name: jnp.zeros(w.shape, jnp.float32) for name, w in weights.items()}
    by_weights, by_x = lax.scan(take, none_yet, (x, dy))
    return (by_x, *(by_weights[name].astype(jnp.bfloat16) for name in NAMES))
```

```python
import functools

import jax
import jax.numpy as jnp
import numpy as np
from jax import lax
from jax.experimental import pallas as pl
from jax.experimental.pallas import tpu as pltpu
from jax.sharding import PartitionSpec as P

HEAD = 128
THETA = 10000
LOG2E = 1.4426950408889634
NEG = -1e30
EPS = 1e-6
WIDE = 512
F32, BF16 = jnp.float32, jnp.bfloat16
VMEM = 60 * 2**20
FWD = dict(bq=512, bk=512, wide=512, diag=256)
BWD = dict(bq=512, bk=512, wide=512, diag=256)
TB = 512


def _dot(a, b, ca=1, cb=0):
    return lax.dot_general(a, b, (((ca,), (cb,)), ((), ())), preferred_element_type=F32)


def _params(n=1):
    return pltpu.CompilerParams(dimension_semantics=("arbitrary",) * n, vmem_limit_bytes=VMEM)


def _whole(shape, at=None):
    at = (0,) * len(shape) if at is None else at
    return pl.BlockSpec(shape, lambda i: at, pipeline_mode=pl.Buffered(1))


def _rows(rows, cols):
    return pl.BlockSpec((rows, cols), lambda i: (i, 0))


def _cost(flops, bytes_accessed, transcendentals=0):
    return pl.CostEstimate(flops=int(flops), bytes_accessed=int(bytes_accessed), transcendentals=int(transcendentals))


def _norm(h):
    wide = h.astype(F32)
    scale = lax.rsqrt(jnp.mean(wide * wide, -1, keepdims=True) + EPS)
    return wide, scale, (wide * scale).astype(BF16)


def _norm_back(d, wide, scale):
    return scale * d - wide * (scale * scale * scale * jnp.mean(d * wide, -1, keepdims=True))


def _turns(tab):
    first = lax.broadcasted_iota(jnp.int32, tab.shape, 1) < HEAD // 2
    other = pltpu.roll(tab, HEAD // 2, 1)
    return jnp.where(first, tab, other), jnp.where(first, -other, tab)


def _matrix(piece):
    return piece.reshape(-1, piece.shape[-1])


def _attend(q_ref, k_ref, v_ref, o_ref, lse_ref, top_s, mix_s, vt_s, *, bq, bk, wide, diag, heads):
    iq = pl.program_id(0)
    scale = HEAD**-0.5
    e = scale * LOG2E
    tokens = k_ref.shape[0]

    @pl.when(iq == 0)
    def _():
        vt_s[:HEAD, :] = v_ref[...].T
        vt_s[HEAD:, :] = jnp.ones((vt_s.shape[0] - HEAD, tokens), BF16)

    top_s[...] = jnp.full(top_s.shape, NEG, F32)
    mix_s[...] = jnp.zeros(mix_s.shape, F32)

    def run(start, pieces):
        scores = [_dot(k_ref[pl.ds(start, keys), :], q_ref[at : at + w, n * HEAD : (n + 1) * HEAD], 1, 1) for n, at, w, keys, _ in pieces]
        weights, keeps = [], []
        for (n, at, w, keys, masked), s in zip(pieces, scores):
            here = slice(n * bq + at, n * bq + at + w)
            if masked:
                gap = lax.broadcasted_iota(jnp.int32, (keys, w), 1) + at - lax.broadcasted_iota(jnp.int32, (keys, w), 0)
                s = jnp.where(gap >= 0, s, 2 * NEG)
            old = top_s[:, here]
            top = jnp.maximum(old, s.max(axis=0, keepdims=True))
            top_s[:, here] = top
            weights.append(jnp.exp2((s - top) * e).astype(BF16))
            keeps.append(jnp.exp2((old - top) * e))
        for (n, at, w, keys, _), p, keep in zip(pieces, weights, keeps):
            here = slice(n * bq + at, n * bq + at + w)
            mix_s[:, here] = mix_s[:, here] * keep + _dot(vt_s[:, pl.ds(start, keys)], p)

    lax.fori_loop(0, iq * (bq // bk), lambda j, _: run(pl.multiple_of(j * bk, bk), [(n, at, wide, bk, False) for n in range(heads) for at in range(0, bq, wide)]), None)
    run(pl.multiple_of(iq * bq, bq), [(n, at, diag, at + diag, True) for n in range(heads) for at in range(0, bq, diag)])
    for n in range(heads):
        here = slice(n * bq, (n + 1) * bq)
        total = mix_s[HEAD : HEAD + 1, here]
        o_ref[:, n * HEAD : (n + 1) * HEAD] = (mix_s[:HEAD, here] * (1 / total)).T.astype(BF16)
        lse_ref[n : n + 1, :] = top_s[:, here] * e + jnp.log2(total)


def attend(q, k, v):
    tokens, width = q.shape
    heads = width // HEAD
    bq = FWD["bq"]
    return pl.pallas_call(
        functools.partial(_attend, heads=heads, **FWD),
        grid=(tokens // bq,),
        in_specs=[_rows(bq, width), _whole((tokens, HEAD)), _whole((tokens, HEAD))],
        out_specs=[_rows(bq, width), pl.BlockSpec((heads, bq), lambda i: (0, i))],
        scratch_shapes=[pltpu.VMEM((1, heads * bq), F32), pltpu.VMEM((HEAD + 8, heads * bq), F32), pltpu.VMEM((HEAD + 8, tokens), BF16)],
        out_shape=[jax.ShapeDtypeStruct((tokens, width), BF16), jax.ShapeDtypeStruct((heads, tokens), F32)],
        compiler_params=_params(),
        cost_estimate=_cost(4 * tokens * tokens * width, 4 * tokens * width, tokens * tokens * heads),
        name="attend",
    )(q, k, v)


def _attend_back(q_ref, k_ref, v_ref, do_ref, lse_ref, delta_ref, dq_ref, dk_ref, dv_ref, dq_s, dk_s, dv_s, kt_s, *, bq, bk, wide, diag, heads):
    iq = pl.program_id(0)
    scale = HEAD**-0.5
    e = scale * LOG2E

    @pl.when(iq == 0)
    def _():
        dk_s[...] = jnp.zeros_like(dk_s)
        dv_s[...] = jnp.zeros_like(dv_s)
        kt_s[...] = k_ref[...].T

    dq_s[...] = jnp.zeros_like(dq_s)

    def run(start, pieces):
        qs = [q_ref[at : at + w, n * HEAD : (n + 1) * HEAD] for n, at, w, _, _ in pieces]
        dos = [do_ref[at : at + w, n * HEAD : (n + 1) * HEAD] for n, at, w, _, _ in pieces]
        scores = [_dot(k_ref[pl.ds(start, piece[3]), :], x, 1, 1) for piece, x in zip(pieces, qs)]
        dps = [_dot(v_ref[pl.ds(start, piece[3]), :], x, 1, 1) for piece, x in zip(pieces, dos)]
        for i, (n, at, w, keys, masked) in enumerate(pieces):
            p = jnp.exp2(scores[i] * e - lse_ref[n : n + 1, at : at + w])
            if masked:
                gap = lax.broadcasted_iota(jnp.int32, (keys, w), 1) + at - lax.broadcasted_iota(jnp.int32, (keys, w), 0)
                p = jnp.where(gap >= 0, p, 0.0)
            ds = (p * (dps[i] - delta_ref[n : n + 1, at : at + w])).astype(BF16)
            dv_s[pl.ds(start, keys), :] += _dot(p.astype(BF16), dos[i])
            dk_s[pl.ds(start, keys), :] += _dot(ds, qs[i])
            dq_s[:, n * bq + at : n * bq + at + w] += _dot(kt_s[:, pl.ds(start, keys)], ds)

    lax.fori_loop(0, iq * (bq // bk), lambda j, _: run(pl.multiple_of(j * bk, bk), [(n, at, wide, bk, False) for n in range(heads) for at in range(0, bq, wide)]), None)
    run(pl.multiple_of(iq * bq, bq), [(n, at, diag, at + diag, True) for n in range(heads) for at in range(0, bq, diag)])
    for n in range(heads):
        dq_ref[:, n * HEAD : (n + 1) * HEAD] = (dq_s[:, n * bq : (n + 1) * bq] * scale).T.astype(BF16)

    @pl.when(iq == pl.num_programs(0) - 1)
    def _():
        dk_ref[...] = (dk_s[...] * scale).astype(BF16)
        dv_ref[...] = dv_s[...].astype(BF16)


def attend_back(q, k, v, d_out, lse, delta):
    tokens, width = q.shape
    heads = width // HEAD
    bq = BWD["bq"]
    stats = pl.BlockSpec((heads, bq), lambda i: (0, i))
    keys = _whole((tokens, HEAD))
    return pl.pallas_call(
        functools.partial(_attend_back, heads=heads, **BWD),
        grid=(tokens // bq,),
        in_specs=[_rows(bq, width), keys, keys, _rows(bq, width), stats, stats],
        out_specs=[_rows(bq, width), pl.BlockSpec((tokens, HEAD), lambda i: (0, 0)), pl.BlockSpec((tokens, HEAD), lambda i: (0, 0))],
        scratch_shapes=[pltpu.VMEM((HEAD, heads * bq), F32), pltpu.VMEM((tokens, HEAD), F32), pltpu.VMEM((tokens, HEAD), F32), pltpu.VMEM((HEAD, tokens), BF16)],
        out_shape=[jax.ShapeDtypeStruct((tokens, width), BF16), jax.ShapeDtypeStruct((tokens, HEAD), BF16), jax.ShapeDtypeStruct((tokens, HEAD), BF16)],
        compiler_params=_params(),
        cost_estimate=_cost(10 * tokens * tokens * width, 8 * tokens * width, tokens * tokens * heads),
        name="attend_back",
    )(q, k, v, d_out, lse, delta)


def _project(b, wq, wkv, tab_ref, q_ref, k_ref, v_ref):
    cos, sin = _turns(tab_ref[...])

    def turned(t):
        t = t.astype(BF16).astype(F32)
        return (t * cos + pltpu.roll(t, HEAD // 2, 1) * sin).astype(BF16)

    q = _dot(b, wq)
    for n in range(q.shape[1] // HEAD):
        q_ref[:, n * HEAD : (n + 1) * HEAD] = turned(q[:, n * HEAD : (n + 1) * HEAD])
    kv = _dot(b, wkv)
    k_ref[...] = turned(kv[:, :HEAD])
    v_ref[...] = kv[:, HEAD:].astype(BF16)


def _before(h_ref, wq_ref, wkv_ref, tab_ref, q_ref, k_ref, v_ref):
    _project(_norm(h_ref[...])[2], _matrix(wq_ref[...]), _matrix(wkv_ref[...]), tab_ref, q_ref, k_ref, v_ref)


def _qkv_shapes(tokens, width):
    return [jax.ShapeDtypeStruct((tokens, width), BF16), jax.ShapeDtypeStruct((tokens, HEAD), BF16), jax.ShapeDtypeStruct((tokens, HEAD), BF16)]


def _qkv_specs(width):
    return [_rows(TB, width), _rows(TB, HEAD), _rows(TB, HEAD)]


def _qkv_weights(n, rows, width):
    return [_whole((n, rows, width)), _whole((n, rows, 2 * HEAD), (0, 0, width // (2 * HEAD)))]


def before(h, qkv, tab, width):
    tokens, d = h.shape
    n, rows = qkv.shape[:2]
    return pl.pallas_call(
        _before,
        grid=(tokens // TB,),
        in_specs=[_rows(TB, d), *_qkv_weights(n, rows, width), _rows(TB, HEAD)],
        out_specs=_qkv_specs(width),
        out_shape=_qkv_shapes(tokens, width),
        compiler_params=_params(),
        cost_estimate=_cost(2 * tokens * d * (width + 2 * HEAD), 4 * tokens * d),
        name="before",
    )(h, qkv, qkv, tab)


def _placed(me_ref, *refs):
    n = len(refs) - 1
    for s in range(n):
        refs[n][lax.rem(me_ref[0] - s + n, n)] = refs[s][...]


def placed(me, parts):
    n, shape = len(parts), parts[0].shape
    return pl.pallas_call(
        _placed,
        grid_spec=pltpu.PrefetchScalarGridSpec(
            num_scalar_prefetch=1,
            grid=(1,),
            in_specs=[pl.BlockSpec(shape, lambda i, _: (0, 0))] * n,
            out_specs=pl.BlockSpec((n, *shape), lambda i, _: (0, 0, 0)),
        ),
        out_shape=jax.ShapeDtypeStruct((n, *shape), parts[0].dtype),
        compiler_params=_params(),
        name="placed",
    )(me, *parts)


def _between(h_ref, o_ref, wd_ref, wg_ref, wu_ref, wo_ref, wq_ref, wkv_ref, tab_ref, h1_ref, h2_ref, q_ref, k_ref, v_ref):
    h1 = (h_ref[...].astype(F32) + _dot(o_ref[...], _matrix(wo_ref[...])).astype(BF16).astype(F32)).astype(BF16)
    h1_ref[...] = h1
    b = _norm(h1)[2]
    rows = wo_ref.shape[1]
    total = None
    for c in range(wg_ref.shape[1] // rows):
        gate = _dot(b, _matrix(wg_ref[:, c * rows : (c + 1) * rows, :]))
        up = _dot(b, _matrix(wu_ref[:, c * rows : (c + 1) * rows, :]))
        act = (gate * (1 / (1 + jnp.exp(-gate))) * up).astype(BF16)
        part = _dot(act, _matrix(wd_ref[...])[c * WIDE : (c + 1) * WIDE, :])
        total = part if total is None else total + part
    h2 = (h1.astype(F32) + total.astype(BF16).astype(F32)).astype(BF16)
    h2_ref[...] = h2
    _project(_norm(h2)[2], _matrix(wq_ref[...]), _matrix(wkv_ref[...]), tab_ref, q_ref, k_ref, v_ref)


def _layer_specs(n, rows, ff_rows):
    return [_whole((n, ff_rows, WIDE), (0, i, 0)) for i in range(3)] + [_whole((n, rows, WIDE), (0, 3 * ff_rows // rows, 0))]


def _next_specs(n, rows, ff_rows):
    at = 3 * ff_rows // rows + 1
    return [_whole((n, rows, WIDE), (0, at, 0)), _whole((n, rows, 2 * HEAD), (0, at + 1, 1))]


def between(h, o, this, ff_rows, tab):
    tokens, d = h.shape
    width = o.shape[1]
    n, rows = this.shape[0], d // this.shape[0]
    return pl.pallas_call(
        _between,
        grid=(tokens // TB,),
        in_specs=[_rows(TB, d), _rows(TB, width), *_layer_specs(n, rows, ff_rows), *_next_specs(n, rows, ff_rows), _rows(TB, HEAD)],
        out_specs=[_rows(TB, d), _rows(TB, d), *_qkv_specs(width)],
        out_shape=[jax.ShapeDtypeStruct((tokens, d), BF16), jax.ShapeDtypeStruct((tokens, d), BF16), *_qkv_shapes(tokens, width)],
        compiler_params=_params(),
        cost_estimate=_cost(2 * tokens * d * (2 * width + 2 * HEAD + 3 * n * ff_rows), 10 * tokens * d),
        name="between",
    )(h, o, this, this, this, this, this, this, tab)


def _mlp_back(h_ref, o_ref, dy_ref, wd_ref, wg_ref, wu_ref, wo_ref, dh_ref, do_ref, delta_ref, grad_ref, ag_s, au_s, ad_s, ao_s, *, joined):
    i = pl.program_id(0)
    n, rows, ff_rows = wo_ref.shape[0], wo_ref.shape[1], wg_ref.shape[1]

    @pl.when(i == 0)
    def _():
        for s in (ag_s, au_s, ad_s, ao_s):
            s[...] = jnp.zeros_like(s)

    wo = _matrix(wo_ref[...])
    o, dy = o_ref[...], dy_ref[...]
    h1 = h_ref[...]
    if joined:
        h1 = (h1.astype(F32) + _dot(o, wo).astype(BF16).astype(F32)).astype(BF16)
    wide, scale, b = _norm(h1)
    db = None
    for c in range(ff_rows // rows):
        here = slice(c * WIDE, (c + 1) * WIDE)
        wg, wu = (_matrix(w[:, c * rows : (c + 1) * rows, :]) for w in (wg_ref, wu_ref))
        gate, up = _dot(b, wg), _dot(b, wu)
        dact = _dot(dy, _matrix(wd_ref[...])[here, :], 1, 1).astype(BF16).astype(F32)
        sig = 1 / (1 + jnp.exp(-gate))
        silu = gate * sig
        act = (silu * up).astype(BF16)
        dup = (dact * silu).astype(BF16)
        dgate = (dact * up * (sig + silu * (1 - sig))).astype(BF16)
        ad_s[:, here] += _dot(dy, act, 0, 0)
        ag_s[:, here] += _dot(b, dgate, 0, 0)
        au_s[:, here] += _dot(b, dup, 0, 0)
        part = _dot(dgate, wg, 1, 1) + _dot(dup, wu, 1, 1)
        db = part if db is None else db + part
    dh = (dy.astype(F32) + _norm_back(db.astype(BF16).astype(F32), wide, scale).astype(BF16).astype(F32)).astype(BF16)
    dh_ref[...] = dh
    do = _dot(dh, wo, 1, 1).astype(BF16)
    do_ref[...] = do
    ao_s[...] += _dot(o, dh, 0, 0)
    ones = jnp.ones((8, HEAD), BF16)
    for m in range(o.shape[1] // HEAD):
        here = slice(m * HEAD, (m + 1) * HEAD)
        both = do[:, here].astype(F32) * o[:, here].astype(F32)
        high = both.astype(BF16)
        low = (both - high.astype(F32)).astype(BF16)
        delta_ref[m : m + 1, :] = (_dot(ones, high, 1, 1) + _dot(ones, low, 1, 1))[:1, :]

    @pl.when(i == pl.num_programs(0) - 1)
    def _():
        half = min(rows, HEAD)
        for j in range(0, n * ff_rows, HEAD):
            t = ad_s[:, j : j + HEAD].T.astype(BF16)
            for at in range(0, HEAD, half):
                to = (j + at) % ff_rows
                grad_ref[(j + at) // ff_rows, to : to + half, :] = t[at : at + half, :]
        for m in range(n):
            mine = slice(m * rows, (m + 1) * rows)
            for c in range(ff_rows // rows):
                here = slice(c * WIDE, (c + 1) * WIDE)
                grad_ref[m, ff_rows + c * rows : ff_rows + (c + 1) * rows, :] = ag_s[mine, here].astype(BF16)
                grad_ref[m, 2 * ff_rows + c * rows : 2 * ff_rows + (c + 1) * rows, :] = au_s[mine, here].astype(BF16)
            grad_ref[m, 3 * ff_rows :, :] = ao_s[mine, :].astype(BF16)


def mlp_back(h, o, dy, this, ff_rows, joined):
    tokens, d = h.shape
    width = o.shape[1]
    heads = width // HEAD
    n, rows = this.shape[0], d // this.shape[0]
    ff = n * ff_rows
    return pl.pallas_call(
        functools.partial(_mlp_back, joined=joined),
        grid=(tokens // TB,),
        in_specs=[_rows(TB, d), _rows(TB, width), _rows(TB, d), *_layer_specs(n, rows, ff_rows)],
        out_specs=[_rows(TB, d), _rows(TB, width), pl.BlockSpec((heads, TB), lambda i: (0, i)), _whole((n, 3 * ff_rows + rows, WIDE))],
        scratch_shapes=[pltpu.VMEM((d, ff), F32), pltpu.VMEM((d, ff), F32), pltpu.VMEM((d, ff), F32), pltpu.VMEM((width, d), F32)],
        out_shape=[jax.ShapeDtypeStruct((tokens, d), BF16), jax.ShapeDtypeStruct((tokens, width), BF16), jax.ShapeDtypeStruct((heads, tokens), F32),
                   jax.ShapeDtypeStruct((n, 3 * ff_rows + rows, WIDE), BF16)],
        compiler_params=_params(),
        cost_estimate=_cost(2 * tokens * d * (8 * ff + 2 * width), 10 * tokens * d),
        name="mlp_back",
    )(h, o, dy, this, this, this, this)


def _before_back(me_ref, h_ref, dh_ref, dq_ref, dk_ref, dv_ref, tab_ref, wq_ref, wkv_ref, dx_ref, *rest):
    *parts, sum_s = rest
    i = pl.program_id(0)
    n, rows = wq_ref.shape[:2]
    width = dq_ref.shape[1]

    @pl.when(i == 0)
    def _():
        sum_s[...] = jnp.zeros_like(sum_s)

    cos, sin = _turns(tab_ref[...])

    def back(t):
        t = t.astype(F32)
        return (t * cos - pltpu.roll(t, HEAD // 2, 1) * sin).astype(BF16)

    wide, scale, a = _norm(h_ref[...])
    dq = jnp.concatenate([back(dq_ref[:, m * HEAD : (m + 1) * HEAD]) for m in range(width // HEAD)], axis=1)
    dkv = jnp.concatenate([back(dk_ref[...]), dv_ref[...]], axis=1)
    da = _dot(dq, _matrix(wq_ref[...]), 1, 1) + _dot(dkv, _matrix(wkv_ref[...]), 1, 1)
    sum_s[:, :width] += _dot(a, dq, 0, 0)
    sum_s[:, width:] += _dot(a, dkv, 0, 0)
    dx_ref[...] = (dh_ref[...].astype(F32) + _norm_back(da.astype(BF16).astype(F32), wide, scale).astype(BF16).astype(F32)).astype(BF16)

    @pl.when(i == pl.num_programs(0) - 1)
    def _():
        for s in range(n):
            parts[s][...] = sum_s[pl.ds(pl.multiple_of(lax.rem(me_ref[0] + s, n) * rows, rows), rows), :].astype(BF16)


def before_back(me, h, dh, dq, dk, dv, tab, wq, wkv, specs):
    tokens, d = h.shape
    width = dq.shape[1]
    n, rows = wq.shape[0], d // wq.shape[0]
    given = [_rows(TB, d), _rows(TB, d), _rows(TB, width), _rows(TB, HEAD), _rows(TB, HEAD), _rows(TB, HEAD), *specs]
    for_me = lambda spec: pl.BlockSpec(spec.block_shape, lambda i, _: spec.index_map(i), pipeline_mode=spec.pipeline_mode)
    part = (rows, width + 2 * HEAD)
    return pl.pallas_call(
        _before_back,
        grid_spec=pltpu.PrefetchScalarGridSpec(
            num_scalar_prefetch=1,
            grid=(tokens // TB,),
            in_specs=[for_me(spec) for spec in given],
            out_specs=[for_me(_rows(TB, d)), *[for_me(_whole(part))] * n],
            scratch_shapes=[pltpu.VMEM((d, width + 2 * HEAD), F32)],
        ),
        out_shape=[jax.ShapeDtypeStruct((tokens, d), BF16), *[jax.ShapeDtypeStruct(part, BF16)] * n],
        compiler_params=_params(),
        cost_estimate=_cost(4 * tokens * d * (width + 2 * HEAD), 8 * tokens * d),
        name="before_back",
    )(me, h, dh, dq, dk, dv, tab, wq, wkv)


def _table(tokens):
    half = HEAD // 2
    angle = np.arange(tokens, dtype=np.float32)[:, None] * np.float32(THETA) ** (-np.arange(half, dtype=np.float32) / np.float32(half))
    return np.concatenate([np.cos(angle), np.sin(angle)], 1).astype(np.float32)


def _cut(w):
    return [w[:, at : at + WIDE] for at in range(0, w.shape[1], WIDE)]


def solution(mesh):
    devices = mesh.shape["dp"]

    def gather(pieces):
        return lax.all_gather(jnp.concatenate(pieces, axis=0), "dp", axis=0, tiled=False)

    def scatter(terms):
        return lax.psum_scatter(terms, "dp", scatter_dimension=0, tiled=False)

    def exchange(parts):
        return [lax.ppermute(part, "dp", [(i, (i + s) % devices) for i in range(devices)]) for s, part in enumerate(parts, 1)]

    def step(x, dy, wq, wk, wv, wo, w_gate, w_up, w_down):
        x, dy = x[0], dy[0]
        tokens, _ = x.shape
        rows, ff_rows = wq.shape[1], w_down.shape[1]
        width = wq.shape[2]
        tab = jnp.asarray(_table(tokens))
        me = lax.axis_index("dp").astype(jnp.int32).reshape(1)
        own = jnp.concatenate([wq[0], wk[0], wv[0]], axis=1)
        qkv = placed(me, [own, *exchange([own] * (devices - 1))])
        pairs = jnp.concatenate([wk[0], wv[0], wk[1], wv[1]], axis=1)
        one = gather([w_down[0], *_cut(w_gate[0]), *_cut(w_up[0]), wo[0], wq[1], pairs])
        two = gather([w_down[1], *_cut(w_gate[1]), *_cut(w_up[1]), wo[1]])

        q0, k0, v0 = before(x, qkv, tab, width)
        o0, lse0 = attend(q0, k0, v0)
        h1, h2, q1, k1, v1 = between(x, o0, one, ff_rows, tab)
        o1, lse1 = attend(q1, k1, v1)

        def summed(parts):
            return sum(t.astype(F32) for t in (parts[0], *exchange(parts[1:]))).astype(BF16)

        dh, do, delta, grads1 = mlp_back(h2, o1, dy, two, ff_rows, True)
        sums1 = scatter(grads1)
        dq, dk, dv = attend_back(q1, k1, v1, do, lse1, delta)
        dh, *parts = before_back(me, h2, dh, dq, dk, dv, tab, one, one, _next_specs(devices, rows, ff_rows))
        qkv1 = summed(parts)
        dh, do, delta, grads0 = mlp_back(h1, o0, dh, one, ff_rows, False)
        sums0 = scatter(grads0)
        dq, dk, dv = attend_back(q0, k0, v0, do, lse0, delta)
        dx, *parts = before_back(me, x, dh, dq, dk, dv, tab, qkv, qkv, _qkv_weights(devices, rows, width))
        qkv0 = summed(parts)

        def joined(sums, i):
            return jnp.concatenate([sums[ff_rows * i + rows * c : ff_rows * i + rows * (c + 1)] for c in range(ff_rows // rows)], axis=1)

        both = lambda f: jnp.stack([f(sums0), f(sums1)])
        apart = lambda start, size: jnp.stack([t[:, start : start + size] for t in (qkv0, qkv1)])
        return (
            dx[None],
            apart(0, width),
            apart(width, HEAD),
            apart(width + HEAD, HEAD),
            both(lambda s: s[3 * ff_rows : 3 * ff_rows + rows]),
            both(lambda s: joined(s, 1)),
            both(lambda s: joined(s, 2)),
            both(lambda s: s[:ff_rows]),
        )

    states, cut = P(("rep", "dp"), None, None), P(None, "dp", None)

    return jax.shard_map(
        step,
        mesh=mesh,
        in_specs=(states, states) + (cut,) * 7,
        out_specs=(states,) + (P("rep", "dp", None),) * 7,
        check_vma=False,
    )
```
